32 devices in a mesh: gx: 4 (over y, x), gy: 4 (over z), gz: 2 (over core).
Axes of the slice: x: 2, y: 2, z: 4, core: 2. Of those that a mesh axis runs over, the one named last changes fastest.
Arguments:
- residual: float32 [64, 64, 256], P('gx', 'gy', 'gz'), may hold values from -6 to 6
- reaction: float32 [64, 64, 256], P('gx', 'gy', 'gz'), may hold values from 0.0001 to 0.1
- basis_x: float32 [3, 64], P(None, 'gx'), may hold values from -4 to 4
- basis_y: float32 [3, 64], P(None, 'gy'), may hold values from -4 to 4
- basis_z: float32 [3, 256], P(None, 'gz'), may hold values from -4 to 4
- coarse_inverse: float32 [864, 864], P(('gx', 'gy', 'gz')), as said below
Outputs:
- preconditioned: float32 [64, 64, 256], P('gx', 'gy', 'gz')
The draws below stay inside these ranges and needn't reach their ends.
Inputs may be any that keep to these rules, and one draw needn't show every extreme that they name: coarse_inverse is symmetric.
All inputs are finite; a program needn't handle non-finite values.
Results may differ from the reference program's by a relative error of at most 0.0003.
Values sent between devices are 32-bit elements; how exact they have to be, the bound alone decides.
A program may use at most 128 MiB of HBM per device.

```python
import math
import jax
import jax.numpy as jnp
from jax import lax

CX = 16
CY = 16
CZ = 128
MARGIN = 8
LEVELS = 4
SWEEPS = 2
BASIS = 3
NX = 64
NY = 64
NZ = 256
NC = 864
N_GX = 4
N_GY = 4
N_GZ = 2


def draw_coarse_inverse(key, part):
    first_key, second_key = jax.random.split(jax.random.fold_in(key, 11))
    base = 0.03 / math.sqrt(CX * CY * CZ)
    noise = jax.random.normal(first_key, (NC, NC), jnp.float32) * (0.5 * base / math.sqrt(NC))
    symmetric = (noise + noise.T) / math.sqrt(2.0)
    diagonal = jnp.exp(jax.random.uniform(second_key, (NC,), jnp.float32, math.log(0.5), math.log(2.0))) * base
    return symmetric + jnp.diag(diagonal)


def draw_reaction(key, part):
    subkeys = jax.random.split(jax.random.fold_in(key, 23), 3)
    wavevectors = jax.random.uniform(subkeys[0], (8, 3), jnp.float32, -1.0, 1.0) * (2.0 * math.pi / 24.0)
    phases = jax.random.uniform(subkeys[1], (8,), jnp.float32, -math.pi, math.pi)
    coord_first = jnp.arange(NX, dtype=jnp.float32)[:, None, None]
    coord_second = jnp.arange(NY, dtype=jnp.float32)[None, :, None]
    coord_third = jnp.arange(NZ, dtype=jnp.float32)[None, None, :]
    pattern = jnp.zeros((NX, NY, NZ), jnp.float32)
    for term_index in range(8):
        angle_term = wavevectors[term_index, 0] * coord_first + wavevectors[term_index, 1] * coord_second
        angle_term = angle_term + wavevectors[term_index, 2] * coord_third + phases[term_index]
        pattern = pattern + jnp.cos(angle_term)
    smooth_part = jax.nn.sigmoid(0.75 * pattern)
    roughness = jax.random.uniform(subkeys[2], (NX, NY, NZ), jnp.float32, 0.0, 1.0)
    exponent = 2.4 * smooth_part + 0.6 * roughness
    return 0.0001 * jnp.exp(exponent * math.log(10.0))


def level_of(own_key, extent, shards, smallest, largest):
    def one(dim, parts):
        steps = jax.random.uniform(jax.random.fold_in(jax.random.fold_in(own_key, 6), dim), (parts,), jnp.float32, smallest / len(shards), largest / len(shards))
        return jnp.repeat(jnp.exp(steps), extent[dim] // parts).reshape((-1,) + (1,) * (len(extent) - dim - 1))

    level = one(*shards[0])
    for cut in shards[1:]:
        level = level * one(*cut)
    return level


def gaussian(own_key, shape, deviation, bound, pieces=(), kind=jnp.bfloat16):
    drawn = jax.random.normal(own_key, shape, jnp.float32) * deviation
    if len(pieces) > 0:
        drawn = level_of(own_key, shape, pieces, -0.22, 0.18) * drawn
    return jnp.clip(drawn, min=-bound, max=bound).astype(kind)


def setup_inputs(seed: int = 0) -> dict:
    splits = jax.random.split(jax.random.key(seed), 7)
    residual = gaussian(splits[0], (NX, NY, NZ), 1.0, 6.0, ((0, 4), (1, 4), (2, 2)), jnp.float32)
    reaction = draw_reaction(jax.random.fold_in(splits[6], 71), 0)
    basis_x = gaussian(splits[2], (BASIS, NX), 1.0, 4.0, ((1, 4),), jnp.float32)
    basis_y = gaussian(splits[3], (BASIS, NY), 1.0, 4.0, ((1, 4),), jnp.float32)
    basis_z = gaussian(splits[4], (BASIS, NZ), 1.0, 4.0, ((1, 2),), jnp.float32)
    coarse_inverse = draw_coarse_inverse(jax.random.fold_in(splits[6], 71), 0)
    return {"residual": residual, "reaction": reaction, "basis_x": basis_x, "basis_y": basis_y, "basis_z": basis_z, "coarse_inverse": coarse_inverse}


damping = 0.8


def operate(iterate, react, factor):
    padded = jnp.pad(iterate, 1)
    beside = padded[2:, 1:-1, 1:-1] + padded[:-2, 1:-1, 1:-1]
    beside = beside + padded[1:-1, 2:, 1:-1] + padded[1:-1, :-2, 1:-1]
    beside = beside + padded[1:-1, 1:-1, 2:] + padded[1:-1, 1:-1, :-2]
    return factor * (6.0 * iterate - beside) + react * iterate


def smooth(iterate, source, react, inside, factor):
    update = iterate + damping * (source - operate(iterate, react, factor)) / (6.0 * factor + react)
    return update * inside


def coarsen(values):
    first, second, third = values.shape
    return values.reshape(first // 2, 2, second // 2, 2, third // 2, 2).mean(axis=(1, 3, 5))


def refine(values):
    return jnp.repeat(jnp.repeat(jnp.repeat(values, 2, 0), 2, 1), 2, 2)


def vcycle(source, react, inside, levels_down):
    factor = 0.25 ** levels_down
    iterate = jnp.zeros_like(source)
    if levels_down == LEVELS - 1:
        for sweep_count in range(2 * SWEEPS):
            iterate = smooth(iterate, source, react, inside, factor)
        return iterate
    for sweep_count in range(SWEEPS):
        iterate = smooth(iterate, source, react, inside, factor)
    defect = (source - operate(iterate, react, factor)) * inside
    lower = vcycle(coarsen(defect), coarsen(react), inside[::2, ::2, ::2], levels_down + 1)
    iterate = iterate + refine(lower) * inside
    for sweep_count in range(SWEEPS):
        iterate = smooth(iterate, source, react, inside, factor)
    return iterate


def reference(residual, reaction, basis_x, basis_y, basis_z, coarse_inverse):
    highest = lax.Precision.HIGHEST
    pad_res = jnp.pad(residual, MARGIN)
    pad_react = jnp.pad(reaction, MARGIN)
    pad_inside = jnp.pad(jnp.ones_like(residual), MARGIN)
    ext_x = CX + 2 * MARGIN
    ext_y = CY + 2 * MARGIN
    ext_z = CZ + 2 * MARGIN

    def solve_one(number):
        index_x = (number // (N_GY * N_GZ)).astype(jnp.int32)
        index_y = ((number // N_GZ) % N_GY).astype(jnp.int32)
        index_z = (number % N_GZ).astype(jnp.int32)
        starts = (index_x * CX, index_y * CY, index_z * CZ)
        source = lax.dynamic_slice(pad_res, starts, (ext_x, ext_y, ext_z))
        react = lax.dynamic_slice(pad_react, starts, (ext_x, ext_y, ext_z))
        inside = lax.dynamic_slice(pad_inside, starts, (ext_x, ext_y, ext_z))
        solved = vcycle(source, react, inside, 0)
        return solved[MARGIN:MARGIN + CX, MARGIN:MARGIN + CY, MARGIN:MARGIN + CZ]

    blocks = lax.map(solve_one, jnp.arange(N_GX * N_GY * N_GZ, dtype=jnp.int32))
    local = blocks.reshape(N_GX, N_GY, N_GZ, CX, CY, CZ).transpose(0, 3, 1, 4, 2, 5).reshape(NX, NY, NZ)

    grid = residual.reshape(N_GX, CX, N_GY, CY, N_GZ, CZ)
    factor_x = basis_x.reshape(BASIS, N_GX, CX)
    factor_y = basis_y.reshape(BASIS, N_GY, CY)
    factor_z = basis_z.reshape(BASIS, N_GZ, CZ)
    first = jnp.einsum('ckz,ixjykz->ixjyck', factor_z, grid, precision=highest)
    second = jnp.einsum('bjy,ixjyck->ixjbck', factor_y, first, precision=highest)
    third = jnp.einsum('aix,ixjbck->ijkabc', factor_x, second, precision=highest)
    projected = third.reshape(-1)
    coefficients = jnp.dot(coarse_inverse, projected, precision=highest)
    coeff_grid = coefficients.reshape(N_GX, N_GY, N_GZ, BASIS, BASIS, BASIS)
    spread_x = jnp.einsum('ijkabc,aix->ixjkbc', coeff_grid, factor_x, precision=highest)
    spread_y = jnp.einsum('ixjkbc,bjy->ixjykc', spread_x, factor_y, precision=highest)
    spread_z = jnp.einsum('ixjykc,ckz->ixjykz', spread_y, factor_z, precision=highest)
    return local + spread_z.reshape(NX, NY, NZ)
```

```python
import functools

import jax
import jax.numpy as jnp
from jax import lax
from jax.experimental import pallas as pl
from jax.experimental.pallas import tpu as pltpu
from jax.sharding import PartitionSpec as P

MARGIN = 8
LEVELS = 4
SWEEPS = 2
BASIS = 3
DAMPING = 0.8

MESH = pl.DeviceIdType.MESH
AXES = ("gx", "gy", "gz")
HIGHEST = lax.Precision.HIGHEST
SUB = 8
LANES = 128


def dot(left, right, contract=((1,), (0,))):
    return lax.dot_general(
        left, right, (contract, ((), ())), precision=HIGHEST, preferred_element_type=jnp.float32
    )


def iota(shape, dim):
    return lax.broadcasted_iota(jnp.int32, shape, dim)


def one_hot(condition):
    return jnp.where(condition, 1.0, 0.0).astype(jnp.float32)


def quotient(values, divisor):
    return jnp.floor((values.astype(jnp.float32) + 0.5) * (1.0 / divisor)).astype(jnp.int32)


def kernel(
    counts, res_ref, rea_ref, bx_ref, by_ref, bz_ref, inv_ref, out_ref,
    ext, src0, rea0, *scratch,
):
    size_x, size_y, size_z = res_ref.shape
    wide_x, wide_y = size_x + 2 * MARGIN, size_y + 2 * MARGIN
    groups = wide_x // SUB
    levels = []
    position = 0
    for level in range(LEVELS):
        levels.append(scratch[position : position + 7])
        position += 7
    (pall, rows, bar_send, bar_recv, gat_send, gat_recv) = scratch[position:]
    me = [lax.axis_index(axis) for axis in AXES]
    n_basis = BASIS**3

    barrier = pltpu.get_barrier_semaphore()
    greeted = 0
    for dim, axis in enumerate(AXES):
        for step in range(1, counts[dim]):
            pl.semaphore_signal(
                barrier, inc=1,
                device_id={axis: lax.rem(me[dim] + step, counts[dim])}, device_id_type=MESH,
            )
            greeted += 1

    index27 = iota((n_basis, BASIS), 0)
    column27 = iota((n_basis, BASIS), 1)
    digit_a = quotient(index27, BASIS * BASIS)
    digit_ab = quotient(index27, BASIS)
    pick_a = one_hot(digit_a == column27)
    pick_b = one_hot(digit_ab - BASIS * digit_a == column27)
    pick_c = one_hot(index27 - BASIS * digit_ab == column27)
    cells = size_x * size_y
    cell_x = quotient(iota((size_x, cells), 1), size_y)
    cell_y = iota((size_y, cells), 1) - size_y * quotient(iota((size_y, cells), 1), size_y)
    along_x = dot(dot(pick_a, bx_ref[...]), one_hot(cell_x == iota((size_x, cells), 0)))
    along_y = dot(dot(pick_b, by_ref[...]), one_hot(cell_y == iota((size_y, cells), 0)))
    basis_xy = along_x * along_y
    basis_z = dot(pick_c, bz_ref[...])
    flat = res_ref[...].reshape(cells, size_z)
    projected = jnp.sum(dot(basis_xy, flat) * basis_z, axis=1, keepdims=True)
    own_row = jnp.sum(
        jnp.where(iota((n_basis, LANES), 0) == iota((n_basis, LANES), 1), projected, 0.0),
        axis=0, keepdims=True,
    )
    pall[me[0], me[1], me[2]] = own_row
    own_x, own_y = pl.ds(MARGIN, size_x), pl.ds(MARGIN, size_y)
    low, high = pl.ds(0, MARGIN), pl.ds(MARGIN + size_x, MARGIN)
    low_y, high_y = pl.ds(0, MARGIN), pl.ds(MARGIN + size_y, MARGIN)
    last_x, last_y = pl.ds(size_x - MARGIN, MARGIN), pl.ds(size_y - MARGIN, MARGIN)
    ext[0, own_x, own_y, :] = res_ref[...]
    ext[1, own_x, own_y, :] = rea_ref[...]
    has_low = [index > 0 for index in me]
    has_high = [index < count - 1 for index, count in zip(me, counts)]

    def clear(missing, ref, where):
        @pl.when(jnp.logical_not(missing))
        def _():
            ref[where] = jnp.zeros(ref.at[where].shape, jnp.float32)

    whole = slice(None)
    for field in range(2):
        clear(has_low[0], ext, (field, low))
        clear(has_high[0], ext, (field, high))
        clear(has_low[1], ext, (field, whole, low_y))
        clear(has_high[1], ext, (field, whole, high_y))

    row_low, row_high = pl.ds(SUB, MARGIN), pl.ds(SUB + MARGIN + size_z, MARGIN)
    for field in (src0, rea0):
        clear(has_low[2], field, (whole, row_low))
        clear(has_high[2], field, (whole, row_high))

    def zero_pads(ref):
        shape = ref.shape
        ref[:, 0:SUB, :] = jnp.zeros((shape[0], SUB, LANES), jnp.float32)
        ref[:, shape[1] - SUB :, :] = jnp.zeros((shape[0], SUB, LANES), jnp.float32)

    for refs in levels:
        for ref in refs:
            zero_pads(ref)
    zero_pads(src0)
    zero_pads(rea0)

    pl.semaphore_wait(barrier, greeted)

    def gather(dim):
        copies = []
        where = tuple(me[: dim + 1])
        for step in range(1, counts[dim]):
            slot = dim * max(counts) + step
            copies.append(
                pltpu.make_async_remote_copy(
                    src_ref=pall.at[where], dst_ref=pall.at[where],
                    send_sem=gat_send.at[slot], recv_sem=gat_recv.at[slot],
                    device_id={AXES[dim]: lax.rem(me[dim] + step, counts[dim])},
                    device_id_type=MESH,
                )
            )
        for copy in copies:
            copy.start()
        return copies

    def finish(copies):
        for copy in copies:
            copy.wait()

    def shift(slot, axis, upward, source, target):
        dim = AXES.index(axis)
        sends = has_high[dim] if upward else has_low[dim]
        takes = has_low[dim] if upward else has_high[dim]
        to = me[dim] + 1 if upward else me[dim] - 1
        copy = pltpu.make_async_remote_copy(
            src_ref=source, dst_ref=target,
            send_sem=bar_send.at[slot], recv_sem=bar_recv.at[slot],
            device_id={axis: jnp.clip(to, 0, counts[dim] - 1)}, device_id_type=MESH,
        )
        return copy, sends, takes

    def start(entry):
        pl.when(entry[1])(entry[0].start)

    def await_recv(entry):
        pl.when(entry[2])(entry[0].wait_recv)

    def await_send(entry):
        pl.when(entry[1])(entry[0].wait_send)

    gathering = gather(2)
    inputs = (res_ref, rea_ref)
    x_faces, y_faces = [], []
    for field, ref in enumerate(inputs):
        x_faces.append((
            shift(4 * field, "gx", True, ref.at[last_x], ext.at[field, low, own_y]),
            shift(4 * field + 1, "gx", False, ref.at[pl.ds(0, MARGIN)], ext.at[field, high, own_y]),
        ))
        y_faces.append((
            shift(4 * field + 2, "gy", True, ref.at[:, last_y], ext.at[field, own_x, low_y]),
            shift(4 * field + 3, "gy", False, ref.at[:, pl.ds(0, MARGIN)], ext.at[field, own_x, high_y]),
        ))
        for entry in x_faces[-1] + y_faces[-1]:
            start(entry)
    finish(gathering)
    gathering = gather(1)
    near_low, near_high = pl.ds(size_y, MARGIN), pl.ds(MARGIN, MARGIN)
    corners = []
    for field in range(2):
        mine = []
        for side, part in enumerate((low, high)):
            await_recv(x_faces[field][side])
            present = has_low[0] if side == 0 else has_high[0]
            for upward in (True, False):
                slot = 8 + 4 * field + 2 * side + (0 if upward else 1)
                near, far = (near_low, low_y) if upward else (near_high, high_y)
                copy, sends, takes = shift(
                    slot, "gy", upward, ext.at[field, part, near], ext.at[field, part, far]
                )
                entry = (copy, sends & present, takes & present)
                start(entry)
                mine.append(entry)
        corners.append(mine)
        if field == 0:
            finish(gathering)
            gathering = gather(0)
    z_faces = []
    for field, ref in enumerate((src0, rea0)):
        for entry in list(y_faces[field]) + corners[field]:
            await_recv(entry)
        for group in range(SUB):
            block = jnp.concatenate(
                [ext[field, SUB * part + group] for part in range(groups)], axis=0
            )
            ref[group, SUB + MARGIN : SUB + MARGIN + size_z, :] = block.T
        pair = (
            shift(16 + 2 * field, "gz", True, ref.at[:, pl.ds(SUB + size_z, MARGIN)], ref.at[:, row_low]),
            shift(17 + 2 * field, "gz", False, ref.at[:, pl.ds(SUB + MARGIN, MARGIN)], ref.at[:, row_high]),
        )
        for entry in pair:
            start(entry)
        z_faces.extend(pair)
    finish(gathering)

    total = counts[0] * counts[1] * counts[2]
    unknowns = inv_ref.shape[1]
    for number in range(total):
        i, rest = divmod(number, counts[1] * counts[2])
        j, k = divmod(rest, counts[2])
        rows[number : number + 1, :] = pall[i, j, k]
    column = iota((LANES, unknowns), 1)
    spread = one_hot(column - n_basis * quotient(column, n_basis) == iota((LANES, unknowns), 0))
    wide = dot(rows[...], spread)
    owner_low = iota((total, unknowns), 0) * n_basis
    owner_column = iota((total, unknowns), 1)
    owned = (owner_column >= owner_low) & (owner_column < owner_low + n_basis)
    vector = jnp.sum(jnp.where(owned, wide, 0.0), axis=0, keepdims=True)
    coefficients = jnp.sum(inv_ref[...] * vector, axis=1, keepdims=True)
    coarse = dot(basis_xy, coefficients * basis_z, ((0,), (0,)))
    out_ref[...] = coarse.reshape(size_x, size_y, size_z)

    for entry in z_faces:
        await_recv(entry)

    lane = iota((SUB, LANES), 1)
    row = iota((SUB, LANES), 0)
    lane_y = lane & (wide_y - 1)

    def present_lanes():
        ok = (lane >= wide_y) | has_low[0]
        ok = ok & ((lane < LANES - wide_y) | has_high[0])
        ok = ok & ((lane_y >= MARGIN) | has_low[1])
        return ok & ((lane_y < MARGIN + size_y) | has_high[1])

    lanes_in = one_hot(present_lanes())
    wide_z = size_z + 2 * MARGIN

    def inside(tile, level):
        z = tile * SUB + row
        margin = MARGIN >> level
        first = jnp.where(has_low[2], 0, margin)
        end = jnp.where(has_high[2], wide_z >> level, (wide_z >> level) - margin)
        return jnp.where((z >= first) & (z < end), lanes_in, 0.0)

    def each(ref, level, body, most):
        tiles = -(-(wide_z >> level) // SUB)
        step = max(k for k in range(1, most + 1) if tiles % k == 0)

        def loop(index, carry):
            for part in range(step):
                body(index * step + part)
            return carry

        lax.fori_loop(0, tiles // step, loop, 0)

    def beside(ref, level, tile):
        reach = 1 << level
        count = SUB >> level
        at = SUB + tile * SUB
        if not isinstance(tile, int):
            at = pl.multiple_of(at, SUB)
        here = [ref[g, pl.ds(at, SUB), :] for g in range(count)]
        sums = []
        for g in range(count):
            up = ref[g, pl.ds(at + 1, SUB), :] + ref[g, pl.ds(at - 1, SUB), :]
            side = jnp.where(lane_y >= reach, pltpu.roll(here[g], reach, 1), 0.0)
            side = side + jnp.where(lane_y < wide_y - reach, pltpu.roll(here[g], LANES - reach, 1), 0.0)
            if g > 0:
                before = here[g - 1]
            else:
                before = jnp.where(lane >= wide_y, pltpu.roll(here[count - 1], wide_y, 1), 0.0)
            if g < count - 1:
                after = here[g + 1]
            else:
                after = jnp.where(lane < LANES - wide_y, pltpu.roll(here[0], LANES - wide_y, 1), 0.0)
            sums.append((up + side) + (before + after))
        return at, here, sums

    def prepare(level):
        source, react, weight, first, _, _, _ = levels_of[level]
        factor = 0.25**level

        def body(tile):
            at = pl.multiple_of(SUB + tile * SUB, SUB)
            mask = inside(tile, level) * DAMPING
            for g in range(SUB >> level):
                value = mask / (6.0 * factor + react[g, pl.ds(at, SUB), :])
                weight[g, pl.ds(at, SUB), :] = value * factor
                first[g, pl.ds(at, SUB), :] = value * source[g, pl.ds(at, SUB), :]

        each(source, level, body, 3)

    def sweep(level, ref, target):
        _, _, weight, first, _, _, _ = levels_of[level]

        def body(tile):
            at, here, sums = beside(ref, level, tile)
            for g in range(SUB >> level):
                new = (1.0 - DAMPING) * here[g] + first[g, pl.ds(at, SUB), :]
                target[g, pl.ds(at, SUB), :] = new + weight[g, pl.ds(at, SUB), :] * sums[g]

        each(ref, level, body, 2)

    def defect(level, ref, target):
        source, react, _, _, _, _, _ = levels_of[level]
        factor = 0.25**level

        def body(tile):
            at, here, sums = beside(ref, level, tile)
            mask = inside(tile, level) * factor
            for g in range(SUB >> level):
                diagonal = 6.0 * factor + react[g, pl.ds(at, SUB), :]
                value = source[g, pl.ds(at, SUB), :] - diagonal * here[g]
                target[g, pl.ds(at, SUB), :] = value + mask * sums[g]

        each(ref, level, body, 2)

    def coarsen(level, ref, target):
        reach = 1 << level
        odd = (lane & reach) != 0
        tiles = -(-(wide_z >> (level + 1)) // SUB)
        for tile in range(tiles):
            base = SUB + 2 * SUB * tile
            for g in range(SUB >> (level + 1)):
                value = None
                for part in range(2):
                    for phase in range(2):
                        piece = ref[2 * g + part, pl.ds(base + phase, SUB, stride=2), :]
                        value = piece if value is None else value + piece
                other = jnp.where(odd, pltpu.roll(value, reach, 1), pltpu.roll(value, LANES - reach, 1))
                target[g, SUB + tile * SUB : 2 * SUB + tile * SUB, :] = 0.125 * (value + other)

    def refine(level, lower, target):
        tiles = -(-(wide_z >> (level + 1)) // SUB)
        for tile in range(tiles):
            base = SUB + 2 * SUB * tile
            for g in range(SUB >> (level + 1)):
                value = lower[g, SUB + tile * SUB : 2 * SUB + tile * SUB, :]
                for part in range(2):
                    for phase in range(2):
                        where = (2 * g + part, pl.ds(base + phase, SUB, stride=2), whole)
                        target[where] = target[where] + value

    levels_of = [(src0, rea0) + tuple(levels[0][2:])] + [tuple(refs) for refs in levels[1:]]

    def vcycle(level):
        source, react, weight, first, one, two, rest = levels_of[level]
        prepare(level)
        if level == LEVELS - 1:
            now, later = first, one
            for _ in range(2 * SWEEPS - 1):
                sweep(level, now, later)
                now, later = later, (two if later is one else one)
            return now
        now, later = first, one
        for _ in range(SWEEPS - 1):
            sweep(level, now, later)
            now, later = later, (two if later is one else one)
        defect(level, now, rest)
        coarsen(level, rest, levels_of[level + 1][0])
        coarsen(level, react, levels_of[level + 1][1])
        refine(level, vcycle(level + 1), now)
        for _ in range(SWEEPS):
            sweep(level, now, later)
            now, later = later, now
        return now

    solved = vcycle(0)
    for group in range(SUB):
        block = solved[group, SUB + MARGIN : SUB + MARGIN + size_z, :].T
        for part in range(1, groups - 1):
            x = SUB * part + group - MARGIN
            start_at = part * wide_y + MARGIN
            out_ref[x] = out_ref[x] + block[start_at : start_at + size_y, :]

    for field in range(2):
        for entry in x_faces[field] + y_faces[field] + tuple(corners[field]):
            await_send(entry)
    for entry in z_faces:
        await_send(entry)


def shards(counts, residual, reaction, basis_x, basis_y, basis_z, coarse_inverse):
    size_x, size_y, size_z = residual.shape
    wide_x, wide_y, wide_z = size_x + 2 * MARGIN, size_y + 2 * MARGIN, size_z + 2 * MARGIN
    assert wide_x // SUB * wide_y == LANES and wide_x % SUB == 0
    total = counts[0] * counts[1] * counts[2]
    vmem = pl.BlockSpec(memory_space=pltpu.VMEM)
    tall = wide_z + 2 * SUB
    scratch = [
        pltpu.VMEM((2, wide_x, wide_y, size_z), jnp.float32),
        pltpu.VMEM((SUB, tall, LANES), jnp.float32),
        pltpu.VMEM((SUB, tall, LANES), jnp.float32),
    ]
    for level in range(LEVELS):
        rows = -(-(wide_z >> level) // SUB) * SUB + 2 * SUB
        shape = (SUB >> level, rows, LANES) if level else (1, SUB, LANES)
        scratch += [pltpu.VMEM(shape, jnp.float32)] * 2
        shape = (SUB >> level, rows, LANES)
        scratch += [pltpu.VMEM(shape, jnp.float32)] * 5
    scratch += [
        pltpu.VMEM((*counts, 1, LANES), jnp.float32),
        pltpu.VMEM((total, LANES), jnp.float32),
        pltpu.SemaphoreType.DMA((20,)),
        pltpu.SemaphoreType.DMA((20,)),
        pltpu.SemaphoreType.DMA((3 * max(counts),)),
        pltpu.SemaphoreType.DMA((3 * max(counts),)),
    ]
    return pl.pallas_call(
        functools.partial(kernel, counts),
        out_shape=jax.ShapeDtypeStruct(residual.shape, jnp.float32),
        in_specs=[vmem] * 6,
        out_specs=vmem,
        scratch_shapes=scratch,
        compiler_params=pltpu.CompilerParams(collective_id=0, has_side_effects=True),
    )(residual, reaction, basis_x, basis_y, basis_z, coarse_inverse)


def solution(mesh):
    counts = tuple(mesh.shape[axis] for axis in AXES)
    placed = (
        P("gx", "gy", "gz"),
        P("gx", "gy", "gz"),
        P(None, "gx"),
        P(None, "gy"),
        P(None, "gz"),
        P(AXES, None),
    )
    return jax.shard_map(
        functools.partial(shards, counts), mesh=mesh, in_specs=placed,
        out_specs=P(*AXES), check_vma=False,
    )
```

```python
import functools

import jax
import jax.numpy as jnp
from jax import lax
from jax.experimental import pallas as pl
from jax.experimental.pallas import tpu as pltpu
from jax.sharding import PartitionSpec as P

MARGIN = 8
LEVELS = 4
SWEEPS = 2
BASIS = 3
DAMPING = 0.8
MOST = (6, 9, 9, 9)

MESH = pl.DeviceIdType.MESH
AXES = ("gx", "gy", "gz")
HIGHEST = lax.Precision.HIGHEST
SUB = 8
LANES = 128


def dot(left, right, contract=((1,), (0,))):
    return lax.dot_general(
        left, right, (contract, ((), ())), precision=HIGHEST, preferred_element_type=jnp.float32
    )


def iota(shape, dim):
    return lax.broadcasted_iota(jnp.int32, shape, dim)


def one_hot(condition):
    return jnp.where(condition, 1.0, 0.0).astype(jnp.float32)


def quotient(values, divisor):
    return jnp.floor((values.astype(jnp.float32) + 0.5) * (1.0 / divisor)).astype(jnp.int32)


def kernel(
    counts, res_ref, rea_ref, bx_ref, by_ref, bz_ref, inv_ref, out_ref,
    ext, src0, rea0, inverse, load_sem, *scratch,
):
    size_x, size_y, size_z = res_ref.shape
    wide_x, wide_y = size_x + 2 * MARGIN, size_y + 2 * MARGIN
    groups = wide_x // SUB
    levels = []
    position = 0
    for level in range(LEVELS):
        levels.append(scratch[position : position + 7])
        position += 7
    (pall, rows, bar_send, bar_recv, gat_send, gat_recv) = scratch[position:]
    me = [lax.axis_index(axis) for axis in AXES]
    n_basis = BASIS**3

    barrier = pltpu.get_barrier_semaphore()
    greeted = 0
    for dim, axis in enumerate(AXES):
        for step in range(1, counts[dim]):
            pl.semaphore_signal(
                barrier, inc=1,
                device_id={axis: lax.rem(me[dim] + step, counts[dim])}, device_id_type=MESH,
            )
            greeted += 1

    own_x, own_y = pl.ds(MARGIN, size_x), pl.ds(MARGIN, size_y)
    loads = [
        pltpu.make_async_copy(res_ref, ext.at[0, own_x, own_y], load_sem.at[0]),
        pltpu.make_async_copy(rea_ref, ext.at[1, own_x, own_y], load_sem.at[1]),
        pltpu.make_async_copy(inv_ref, inverse, load_sem.at[2]),
    ]
    for load in loads:
        load.start()

    index27 = iota((n_basis, BASIS), 0)
    column27 = iota((n_basis, BASIS), 1)
    digit_a = quotient(index27, BASIS * BASIS)
    digit_ab = quotient(index27, BASIS)
    pick_a = one_hot(digit_a == column27)
    pick_b = one_hot(digit_ab - BASIS * digit_a == column27)
    pick_c = one_hot(index27 - BASIS * digit_ab == column27)
    cells = size_x * size_y
    cell_x = quotient(iota((size_x, cells), 1), size_y)
    cell_y = iota((size_y, cells), 1) - size_y * quotient(iota((size_y, cells), 1), size_y)
    along_x = dot(dot(pick_a, bx_ref[...]), one_hot(cell_x == iota((size_x, cells), 0)))
    along_y = dot(dot(pick_b, by_ref[...]), one_hot(cell_y == iota((size_y, cells), 0)))
    basis_xy = along_x * along_y
    basis_z = dot(pick_c, bz_ref[...])
    loads[0].wait()
    flat = ext[0, own_x, own_y, :].reshape(cells, size_z)
    projected = jnp.sum(dot(basis_xy, flat) * basis_z, axis=1, keepdims=True)
    own_row = jnp.sum(
        jnp.where(iota((n_basis, LANES), 0) == iota((n_basis, LANES), 1), projected, 0.0),
        axis=0, keepdims=True,
    )
    pall[me[0], me[1], me[2]] = own_row
    low, high = pl.ds(0, MARGIN), pl.ds(MARGIN + size_x, MARGIN)
    low_y, high_y = pl.ds(0, MARGIN), pl.ds(MARGIN + size_y, MARGIN)
    last_x, last_y = pl.ds(size_x, MARGIN), pl.ds(size_y, MARGIN)
    first_x, first_y = pl.ds(MARGIN, MARGIN), pl.ds(MARGIN, MARGIN)
    has_low = [index > 0 for index in me]
    has_high = [index < count - 1 for index, count in zip(me, counts)]

    def clear(missing, ref, where):
        @pl.when(jnp.logical_not(missing))
        def _():
            ref[where] = jnp.zeros(ref.at[where].shape, jnp.float32)

    whole = slice(None)
    for field in range(2):
        clear(has_low[0], ext, (field, low))
        clear(has_high[0], ext, (field, high))
        clear(has_low[1], ext, (field, whole, low_y))
        clear(has_high[1], ext, (field, whole, high_y))

    row_low, row_high = pl.ds(SUB, MARGIN), pl.ds(SUB + MARGIN + size_z, MARGIN)
    for field in (src0, rea0):
        clear(has_low[2], field, (whole, row_low))
        clear(has_high[2], field, (whole, row_high))

    def zero_pads(ref):
        shape = ref.shape
        ref[:, 0:SUB, :] = jnp.zeros((shape[0], SUB, LANES), jnp.float32)
        ref[:, shape[1] - SUB :, :] = jnp.zeros((shape[0], SUB, LANES), jnp.float32)

    for refs in levels:
        for ref in refs:
            zero_pads(ref)
    zero_pads(src0)
    zero_pads(rea0)

    loads[1].wait()
    loads[2].wait()
    pl.semaphore_wait(barrier, greeted)

    def gather(dim):
        copies = []
        where = tuple(me[: dim + 1])
        for step in range(1, counts[dim]):
            slot = dim * max(counts) + step
            copies.append(
                pltpu.make_async_remote_copy(
                    src_ref=pall.at[where], dst_ref=pall.at[where],
                    send_sem=gat_send.at[slot], recv_sem=gat_recv.at[slot],
                    device_id={AXES[dim]: lax.rem(me[dim] + step, counts[dim])},
                    device_id_type=MESH,
                )
            )
        for copy in copies:
            copy.start()
        return copies

    def finish(copies):
        for copy in copies:
            copy.wait()

    def shift(slot, axis, upward, source, target):
        dim = AXES.index(axis)
        sends = has_high[dim] if upward else has_low[dim]
        takes = has_low[dim] if upward else has_high[dim]
        to = me[dim] + 1 if upward else me[dim] - 1
        copy = pltpu.make_async_remote_copy(
            src_ref=source, dst_ref=target,
            send_sem=bar_send.at[slot], recv_sem=bar_recv.at[slot],
            device_id={axis: jnp.clip(to, 0, counts[dim] - 1)}, device_id_type=MESH,
        )
        return copy, sends, takes

    def start(entry):
        pl.when(entry[1])(entry[0].start)

    def await_recv(entry):
        pl.when(entry[2])(entry[0].wait_recv)

    def await_send(entry):
        pl.when(entry[1])(entry[0].wait_send)

    gathering = gather(2)
    x_faces, y_faces, corners = {}, {}, {}
    for field in (1, 0):
        x_faces[field] = (
            shift(4 * field, "gx", True, ext.at[field, last_x, own_y], ext.at[field, low, own_y]),
            shift(4 * field + 1, "gx", False, ext.at[field, first_x, own_y], ext.at[field, high, own_y]),
        )
        y_faces[field] = (
            shift(4 * field + 2, "gy", True, ext.at[field, own_x, last_y], ext.at[field, own_x, low_y]),
            shift(4 * field + 3, "gy", False, ext.at[field, own_x, first_y], ext.at[field, own_x, high_y]),
        )
        for entry in x_faces[field] + y_faces[field]:
            start(entry)
    finish(gathering)
    gathering = gather(1)
    near_low, near_high = pl.ds(size_y, MARGIN), pl.ds(MARGIN, MARGIN)
    for field in (1, 0):
        mine = []
        for side, part in enumerate((low, high)):
            await_recv(x_faces[field][side])
            present = has_low[0] if side == 0 else has_high[0]
            for upward in (True, False):
                slot = 8 + 4 * field + 2 * side + (0 if upward else 1)
                near, far = (near_low, low_y) if upward else (near_high, high_y)
                copy, sends, takes = shift(
                    slot, "gy", upward, ext.at[field, part, near], ext.at[field, part, far]
                )
                entry = (copy, sends & present, takes & present)
                start(entry)
                mine.append(entry)
        corners[field] = mine
    finish(gathering)
    gathering = gather(0)
    z_faces = {}
    for field in (1, 0):
        ref = (src0, rea0)[field]
        for entry in list(y_faces[field]) + corners[field]:
            await_recv(entry)
        for group in range(SUB):
            block = jnp.concatenate(
                [ext[field, SUB * part + group] for part in range(groups)], axis=0
            )
            ref[group, SUB + MARGIN : SUB + MARGIN + size_z, :] = block.T
        pair = (
            shift(16 + 2 * field, "gz", True, ref.at[:, pl.ds(SUB + size_z, MARGIN)], ref.at[:, row_low]),
            shift(17 + 2 * field, "gz", False, ref.at[:, pl.ds(SUB + MARGIN, MARGIN)], ref.at[:, row_high]),
        )
        for entry in pair:
            start(entry)
        z_faces[field] = pair

    lane = iota((SUB, LANES), 1)
    row = iota((SUB, LANES), 0)
    lane_y = lane & (wide_y - 1)

    def present_lanes():
        ok = (lane >= wide_y) | has_low[0]
        ok = ok & ((lane < LANES - wide_y) | has_high[0])
        ok = ok & ((lane_y >= MARGIN) | has_low[1])
        return ok & ((lane_y < MARGIN + size_y) | has_high[1])

    lanes_in = one_hot(present_lanes())
    wide_z = size_z + 2 * MARGIN

    def inside(tile, level):
        z = tile * SUB + row
        margin = MARGIN >> level
        first = jnp.where(has_low[2], 0, margin)
        end = jnp.where(has_high[2], wide_z >> level, (wide_z >> level) - margin)
        return jnp.where((z >= first) & (z < end), lanes_in, 0.0)

    def each(level, body):
        tiles = -(-(wide_z >> level) // SUB)
        most = MOST[level]
        step = max(k for k in range(1, most + 1) if tiles % k == 0)

        def loop(index, carry):
            for part in range(step):
                body(index * step + part)
            return carry

        lax.fori_loop(0, tiles // step, loop, 0)

    def beside(ref, level, tile):
        reach = 1 << level
        count = SUB >> level
        at = SUB + tile * SUB
        if not isinstance(tile, int):
            at = pl.multiple_of(at, SUB)
        here = [ref[g, pl.ds(at, SUB), :] for g in range(count)]
        sums = []
        for g in range(count):
            up = ref[g, pl.ds(at + 1, SUB), :] + ref[g, pl.ds(at - 1, SUB), :]
            side = jnp.where(lane_y >= reach, pltpu.roll(here[g], reach, 1), 0.0)
            side = side + jnp.where(lane_y < wide_y - reach, pltpu.roll(here[g], LANES - reach, 1), 0.0)
            if g > 0:
                before = here[g - 1]
            else:
                before = jnp.where(lane >= wide_y, pltpu.roll(here[count - 1], wide_y, 1), 0.0)
            if g < count - 1:
                after = here[g + 1]
            else:
                after = jnp.where(lane < LANES - wide_y, pltpu.roll(here[0], LANES - wide_y, 1), 0.0)
            sums.append((up + side) + (before + after))
        return at, here, sums

    def weigh(level):
        _, react, weight, _, _, _, _ = levels_of[level]
        factor = 0.25**level

        def body(tile):
            at = pl.multiple_of(SUB + tile * SUB, SUB)
            mask = inside(tile, level) * (DAMPING * factor)
            for g in range(SUB >> level):
                weight[g, pl.ds(at, SUB), :] = mask / (6.0 * factor + react[g, pl.ds(at, SUB), :])

        each(level, body)

    def prepare(level):
        source, _, weight, first, _, _, _ = levels_of[level]

        def body(tile):
            at = pl.multiple_of(SUB + tile * SUB, SUB)
            for g in range(SUB >> level):
                value = 4.0**level * weight[g, pl.ds(at, SUB), :]
                first[g, pl.ds(at, SUB), :] = value * source[g, pl.ds(at, SUB), :]

        each(level, body)

    def sweep(level, ref, target):
        _, _, weight, first, _, _, _ = levels_of[level]

        def body(tile):
            at, here, sums = beside(ref, level, tile)
            for g in range(SUB >> level):
                new = (1.0 - DAMPING) * here[g] + first[g, pl.ds(at, SUB), :]
                target[g, pl.ds(at, SUB), :] = new + weight[g, pl.ds(at, SUB), :] * sums[g]

        each(level, body)

    def defect(level, ref, target):
        source, react, _, _, _, _, _ = levels_of[level]
        factor = 0.25**level

        def body(tile):
            at, here, sums = beside(ref, level, tile)
            mask = inside(tile, level) * factor
            for g in range(SUB >> level):
                diagonal = 6.0 * factor + react[g, pl.ds(at, SUB), :]
                value = source[g, pl.ds(at, SUB), :] - diagonal * here[g]
                target[g, pl.ds(at, SUB), :] = value + mask * sums[g]

        each(level, body)

    def coarsen(level, ref, target):
        reach = 1 << level
        odd = (lane & reach) != 0
        tiles = -(-(wide_z >> (level + 1)) // SUB)
        for tile in range(tiles):
            base = SUB + 2 * SUB * tile
            for g in range(SUB >> (level + 1)):
                value = None
                for part in range(2):
                    for phase in range(2):
                        piece = ref[2 * g + part, pl.ds(base + phase, SUB, stride=2), :]
                        value = piece if value is None else value + piece
                other = jnp.where(odd, pltpu.roll(value, reach, 1), pltpu.roll(value, LANES - reach, 1))
                target[g, SUB + tile * SUB : 2 * SUB + tile * SUB, :] = 0.125 * (value + other)

    def refine(level, lower, target):
        tiles = -(-(wide_z >> (level + 1)) // SUB)
        for tile in range(tiles):
            base = SUB + 2 * SUB * tile
            for g in range(SUB >> (level + 1)):
                value = lower[g, SUB + tile * SUB : 2 * SUB + tile * SUB, :]
                for part in range(2):
                    for phase in range(2):
                        where = (2 * g + part, pl.ds(base + phase, SUB, stride=2), whole)
                        target[where] = target[where] + value

    levels_of = [(src0, rea0) + tuple(levels[0][2:])] + [tuple(refs) for refs in levels[1:]]

    def vcycle(level):
        first, one, two, rest = levels_of[level][3:]
        prepare(level)
        if level == LEVELS - 1:
            now, later = first, one
            for _ in range(2 * SWEEPS - 1):
                sweep(level, now, later)
                now, later = later, (two if later is one else one)
            return now
        now, later = first, one
        for _ in range(SWEEPS - 1):
            sweep(level, now, later)
            now, later = later, (two if later is one else one)
        defect(level, now, rest)
        coarsen(level, rest, levels_of[level + 1][0])
        refine(level, vcycle(level + 1), now)
        for _ in range(SWEEPS):
            sweep(level, now, later)
            now, later = later, now
        return now

    for entry in z_faces[1]:
        await_recv(entry)
    for level in range(LEVELS):
        weigh(level)
        if level < LEVELS - 1:
            coarsen(level, levels_of[level][1], levels_of[level + 1][1])
    finish(gathering)

    total = counts[0] * counts[1] * counts[2]
    unknowns = inv_ref.shape[1]
    for number in range(total):
        i, rest = divmod(number, counts[1] * counts[2])
        j, k = divmod(rest, counts[2])
        rows[number : number + 1, :] = pall[i, j, k]
    column = iota((LANES, unknowns), 1)
    spread = one_hot(column - n_basis * quotient(column, n_basis) == iota((LANES, unknowns), 0))
    wide = dot(rows[...], spread)
    owner_low = iota((total, unknowns), 0) * n_basis
    owner_column = iota((total, unknowns), 1)
    owned = (owner_column >= owner_low) & (owner_column < owner_low + n_basis)
    vector = jnp.sum(jnp.where(owned, wide, 0.0), axis=0, keepdims=True)
    coefficients = jnp.sum(inverse[...] * vector, axis=1, keepdims=True)
    coarse = dot(basis_xy, coefficients * basis_z, ((0,), (0,)))
    out_ref[...] = coarse.reshape(size_x, size_y, size_z)

    for entry in z_faces[0]:
        await_recv(entry)
    solved = vcycle(0)
    for group in range(SUB):
        block = solved[group, SUB + MARGIN : SUB + MARGIN + size_z, :].T
        for part in range(1, groups - 1):
            x = SUB * part + group - MARGIN
            start_at = part * wide_y + MARGIN
            out_ref[x] = out_ref[x] + block[start_at : start_at + size_y, :]

    for field in range(2):
        for entry in x_faces[field] + y_faces[field] + tuple(corners[field]) + z_faces[field]:
            await_send(entry)


def shards(counts, residual, reaction, basis_x, basis_y, basis_z, coarse_inverse):
    size_x, size_y, size_z = residual.shape
    wide_x, wide_y, wide_z = size_x + 2 * MARGIN, size_y + 2 * MARGIN, size_z + 2 * MARGIN
    assert wide_x // SUB * wide_y == LANES and wide_x % SUB == 0
    total = counts[0] * counts[1] * counts[2]
    vmem = pl.BlockSpec(memory_space=pltpu.VMEM)
    placed = pl.BlockSpec(memory_space=pl.ANY)
    tall = wide_z + 2 * SUB
    scratch = [
        pltpu.VMEM((2, wide_x, wide_y, size_z), jnp.float32),
        pltpu.VMEM((SUB, tall, LANES), jnp.float32),
        pltpu.VMEM((SUB, tall, LANES), jnp.float32),
        pltpu.VMEM(coarse_inverse.shape, jnp.float32),
        pltpu.SemaphoreType.DMA((3,)),
    ]
    for level in range(LEVELS):
        rows = -(-(wide_z >> level) // SUB) * SUB + 2 * SUB
        shape = (SUB >> level, rows, LANES) if level else (1, SUB, LANES)
        scratch += [pltpu.VMEM(shape, jnp.float32)] * 2
        shape = (SUB >> level, rows, LANES)
        scratch += [pltpu.VMEM(shape, jnp.float32)] * 5
    scratch += [
        pltpu.VMEM((*counts, 1, LANES), jnp.float32),
        pltpu.VMEM((total, LANES), jnp.float32),
        pltpu.SemaphoreType.DMA((20,)),
        pltpu.SemaphoreType.DMA((20,)),
        pltpu.SemaphoreType.DMA((3 * max(counts),)),
        pltpu.SemaphoreType.DMA((3 * max(counts),)),
    ]
    return pl.pallas_call(
        functools.partial(kernel, counts),
        out_shape=jax.ShapeDtypeStruct(residual.shape, jnp.float32),
        in_specs=[placed, placed, vmem, vmem, vmem, placed],
        out_specs=vmem,
        scratch_shapes=scratch,
        compiler_params=pltpu.CompilerParams(collective_id=0, has_side_effects=True),
    )(residual, reaction, basis_x, basis_y, basis_z, coarse_inverse)


def solution(mesh):
    counts = tuple(mesh.shape[axis] for axis in AXES)
    placed = (
        P("gx", "gy", "gz"),
        P("gx", "gy", "gz"),
        P(None, "gx"),
        P(None, "gy"),
        P(None, "gz"),
        P(AXES, None),
    )
    return jax.shard_map(
        functools.partial(shards, counts), mesh=mesh, in_specs=placed,
        out_specs=P(*AXES), check_vma=False,
    )
```

```python
import functools

import jax
import jax.numpy as jnp
from jax import lax
from jax.experimental import pallas as pl
from jax.experimental.pallas import tpu as pltpu
from jax.sharding import PartitionSpec as P

MARGIN = 8
LEVELS = 4
SWEEPS = 2
BASIS = 3
DAMPING = 0.8
MOST = (18, 9, 9, 9)

MESH = pl.DeviceIdType.MESH
AXES = ("gx", "gy", "gz")
HIGHEST = lax.Precision.HIGHEST
SUB = 8
LANES = 128


def dot(left, right, contract=((1,), (0,))):
    return lax.dot_general(
        left, right, (contract, ((), ())), precision=HIGHEST, preferred_element_type=jnp.float32
    )


def iota(shape, dim):
    return lax.broadcasted_iota(jnp.int32, shape, dim)


def one_hot(condition):
    return jnp.where(condition, 1.0, 0.0).astype(jnp.float32)


def quotient(values, divisor):
    return jnp.floor((values.astype(jnp.float32) + 0.5) * (1.0 / divisor)).astype(jnp.int32)


def kernel(
    counts, res_ref, rea_ref, bx_ref, by_ref, bz_ref, inv_ref, out_ref,
    ext, src0, rea0, inverse, load_sem, *scratch,
):
    size_x, size_y, size_z = res_ref.shape
    wide_x, wide_y = size_x + 2 * MARGIN, size_y + 2 * MARGIN
    groups = wide_x // SUB
    levels = []
    position = 0
    for level in range(LEVELS):
        levels.append(scratch[position : position + 7])
        position += 7
    (pall, rows, bar_send, bar_recv, gat_send, gat_recv) = scratch[position:]
    me = [lax.axis_index(axis) for axis in AXES]
    n_basis = BASIS**3

    barrier = pltpu.get_barrier_semaphore()
    greeted = 0
    for dim, axis in enumerate(AXES):
        for step in range(1, counts[dim]):
            pl.semaphore_signal(
                barrier, inc=1,
                device_id={axis: lax.rem(me[dim] + step, counts[dim])}, device_id_type=MESH,
            )
            greeted += 1

    own_x, own_y = pl.ds(MARGIN, size_x), pl.ds(MARGIN, size_y)
    loads = [
        pltpu.make_async_copy(res_ref, ext.at[0, own_x, own_y], load_sem.at[0]),
        pltpu.make_async_copy(rea_ref, ext.at[1, own_x, own_y], load_sem.at[1]),
        pltpu.make_async_copy(inv_ref, inverse, load_sem.at[2]),
    ]
    for load in loads:
        load.start()

    index27 = iota((n_basis, BASIS), 0)
    column27 = iota((n_basis, BASIS), 1)
    digit_a = quotient(index27, BASIS * BASIS)
    digit_ab = quotient(index27, BASIS)
    pick_a = one_hot(digit_a == column27)
    pick_b = one_hot(digit_ab - BASIS * digit_a == column27)
    pick_c = one_hot(index27 - BASIS * digit_ab == column27)
    cells = size_x * size_y
    cell_x = quotient(iota((size_x, cells), 1), size_y)
    cell_y = iota((size_y, cells), 1) - size_y * quotient(iota((size_y, cells), 1), size_y)
    along_x = dot(dot(pick_a, bx_ref[...]), one_hot(cell_x == iota((size_x, cells), 0)))
    along_y = dot(dot(pick_b, by_ref[...]), one_hot(cell_y == iota((size_y, cells), 0)))
    basis_xy = along_x * along_y
    basis_z = dot(pick_c, bz_ref[...])
    loads[0].wait()
    flat = ext[0, own_x, own_y, :].reshape(cells, size_z)
    projected = jnp.sum(dot(basis_xy, flat) * basis_z, axis=1, keepdims=True)
    own_row = jnp.sum(
        jnp.where(iota((n_basis, LANES), 0) == iota((n_basis, LANES), 1), projected, 0.0),
        axis=0, keepdims=True,
    )
    pall[me[0], me[1], me[2]] = own_row
    low, high = pl.ds(0, MARGIN), pl.ds(MARGIN + size_x, MARGIN)
    low_y, high_y = pl.ds(0, MARGIN), pl.ds(MARGIN + size_y, MARGIN)
    last_x, last_y = pl.ds(size_x, MARGIN), pl.ds(size_y, MARGIN)
    first_x, first_y = pl.ds(MARGIN, MARGIN), pl.ds(MARGIN, MARGIN)
    has_low = [index > 0 for index in me]
    has_high = [index < count - 1 for index, count in zip(me, counts)]

    def clear(missing, ref, where):
        @pl.when(jnp.logical_not(missing))
        def _():
            ref[where] = jnp.zeros(ref.at[where].shape, jnp.float32)

    whole = slice(None)
    for field in range(2):
        clear(has_low[0], ext, (field, low))
        clear(has_high[0], ext, (field, high))
        clear(has_low[1], ext, (field, whole, low_y))
        clear(has_high[1], ext, (field, whole, high_y))

    row_low, row_high = pl.ds(SUB, MARGIN), pl.ds(SUB + MARGIN + size_z, MARGIN)
    for field in (src0, rea0):
        clear(has_low[2], field, (whole, row_low))
        clear(has_high[2], field, (whole, row_high))

    def zero_pads(ref):
        shape = ref.shape
        ref[:, 0:SUB, :] = jnp.zeros((shape[0], SUB, LANES), jnp.float32)
        ref[:, shape[1] - SUB :, :] = jnp.zeros((shape[0], SUB, LANES), jnp.float32)

    for refs in levels:
        for ref in refs:
            zero_pads(ref)
    zero_pads(src0)
    zero_pads(rea0)

    loads[1].wait()
    loads[2].wait()
    pl.semaphore_wait(barrier, greeted)

    def gather(dim):
        copies = []
        where = tuple(me[: dim + 1])
        for step in range(1, counts[dim]):
            slot = dim * max(counts) + step
            copies.append(
                pltpu.make_async_remote_copy(
                    src_ref=pall.at[where], dst_ref=pall.at[where],
                    send_sem=gat_send.at[slot], recv_sem=gat_recv.at[slot],
                    device_id={AXES[dim]: lax.rem(me[dim] + step, counts[dim])},
                    device_id_type=MESH,
                )
            )
        for copy in copies:
            copy.start()
        return copies

    def finish(copies):
        for copy in copies:
            copy.wait()

    def shift(slot, axis, upward, source, target):
        dim = AXES.index(axis)
        sends = has_high[dim] if upward else has_low[dim]
        takes = has_low[dim] if upward else has_high[dim]
        to = me[dim] + 1 if upward else me[dim] - 1
        copy = pltpu.make_async_remote_copy(
            src_ref=source, dst_ref=target,
            send_sem=bar_send.at[slot], recv_sem=bar_recv.at[slot],
            device_id={axis: jnp.clip(to, 0, counts[dim] - 1)}, device_id_type=MESH,
        )
        return copy, sends, takes

    def start(entry):
        pl.when(entry[1])(entry[0].start)

    def await_recv(entry):
        pl.when(entry[2])(entry[0].wait_recv)

    def await_send(entry):
        pl.when(entry[1])(entry[0].wait_send)

    gathering = gather(2)
    x_faces, y_faces, corners = {}, {}, {}
    for field in (1, 0):
        x_faces[field] = (
            shift(4 * field, "gx", True, ext.at[field, last_x, own_y], ext.at[field, low, own_y]),
            shift(4 * field + 1, "gx", False, ext.at[field, first_x, own_y], ext.at[field, high, own_y]),
        )
        y_faces[field] = (
            shift(4 * field + 2, "gy", True, ext.at[field, own_x, last_y], ext.at[field, own_x, low_y]),
            shift(4 * field + 3, "gy", False, ext.at[field, own_x, first_y], ext.at[field, own_x, high_y]),
        )
        for entry in x_faces[field] + y_faces[field]:
            start(entry)
    finish(gathering)
    gathering = gather(1)
    near_low, near_high = pl.ds(size_y, MARGIN), pl.ds(MARGIN, MARGIN)
    for field in (1, 0):
        mine = []
        for side, part in enumerate((low, high)):
            await_recv(x_faces[field][side])
            present = has_low[0] if side == 0 else has_high[0]
            for upward in (True, False):
                slot = 8 + 4 * field + 2 * side + (0 if upward else 1)
                near, far = (near_low, low_y) if upward else (near_high, high_y)
                copy, sends, takes = shift(
                    slot, "gy", upward, ext.at[field, part, near], ext.at[field, part, far]
                )
                entry = (copy, sends & present, takes & present)
                start(entry)
                mine.append(entry)
        corners[field] = mine
    finish(gathering)
    gathering = gather(0)
    z_faces = {}
    for field in (1, 0):
        ref = (src0, rea0)[field]
        for entry in list(y_faces[field]) + corners[field]:
            await_recv(entry)
        for group in range(SUB):
            block = jnp.concatenate(
                [ext[field, SUB * part + group] for part in range(groups)], axis=0
            )
            ref[group, SUB + MARGIN : SUB + MARGIN + size_z, :] = block.T
        pair = (
            shift(16 + 2 * field, "gz", True, ref.at[:, pl.ds(SUB + size_z, MARGIN)], ref.at[:, row_low]),
            shift(17 + 2 * field, "gz", False, ref.at[:, pl.ds(SUB + MARGIN, MARGIN)], ref.at[:, row_high]),
        )
        for entry in pair:
            start(entry)
        z_faces[field] = pair

    lane = iota((SUB, LANES), 1)
    row = iota((SUB, LANES), 0)
    lane_y = lane & (wide_y - 1)

    def present_lanes():
        ok = (lane >= wide_y) | has_low[0]
        ok = ok & ((lane < LANES - wide_y) | has_high[0])
        ok = ok & ((lane_y >= MARGIN) | has_low[1])
        return ok & ((lane_y < MARGIN + size_y) | has_high[1])

    lanes_in = one_hot(present_lanes())
    wide_z = size_z + 2 * MARGIN

    def inside(tile, level):
        z = tile * SUB + row
        margin = MARGIN >> level
        first = jnp.where(has_low[2], 0, margin)
        end = jnp.where(has_high[2], wide_z >> level, (wide_z >> level) - margin)
        return jnp.where((z >= first) & (z < end), lanes_in, 0.0)

    def each(level, body):
        tiles = -(-(wide_z >> level) // SUB)
        most = MOST[level]
        step = max(k for k in range(1, most + 1) if tiles % k == 0)

        def loop(index, carry):
            for part in range(step):
                body(index * step + part)
            return carry

        lax.fori_loop(0, tiles // step, loop, 0)

    def beside(ref, level, tile):
        reach = 1 << level
        count = SUB >> level
        at = SUB + tile * SUB
        if not isinstance(tile, int):
            at = pl.multiple_of(at, SUB)
        here = [ref[g, pl.ds(at, SUB), :] for g in range(count)]
        sums = []
        for g in range(count):
            up = ref[g, pl.ds(at + 1, SUB), :] + ref[g, pl.ds(at - 1, SUB), :]
            side = jnp.where(lane_y >= reach, pltpu.roll(here[g], reach, 1), 0.0)
            side = side + jnp.where(lane_y < wide_y - reach, pltpu.roll(here[g], LANES - reach, 1), 0.0)
            if g > 0:
                before = here[g - 1]
            else:
                before = jnp.where(lane >= wide_y, pltpu.roll(here[count - 1], wide_y, 1), 0.0)
            if g < count - 1:
                after = here[g + 1]
            else:
                after = jnp.where(lane < LANES - wide_y, pltpu.roll(here[0], LANES - wide_y, 1), 0.0)
            sums.append((up + side) + (before + after))
        return at, here, sums

    def weigh(level):
        _, react, weight, _, _, _, _ = levels_of[level]
        factor = 0.25**level

        def body(tile):
            at = pl.multiple_of(SUB + tile * SUB, SUB)
            mask = inside(tile, level) * (DAMPING * factor)
            for g in range(SUB >> level):
                weight[g, pl.ds(at, SUB), :] = mask / (6.0 * factor + react[g, pl.ds(at, SUB), :])

        each(level, body)

    def prepare(level):
        source, _, weight, first, _, _, _ = levels_of[level]

        def body(tile):
            at = pl.multiple_of(SUB + tile * SUB, SUB)
            for g in range(SUB >> level):
                value = 4.0**level * weight[g, pl.ds(at, SUB), :]
                first[g, pl.ds(at, SUB), :] = value * source[g, pl.ds(at, SUB), :]

        each(level, body)

    def sweep(level, ref, target):
        _, _, weight, first, _, _, _ = levels_of[level]

        def body(tile):
            at, here, sums = beside(ref, level, tile)
            for g in range(SUB >> level):
                new = (1.0 - DAMPING) * here[g] + first[g, pl.ds(at, SUB), :]
                target[g, pl.ds(at, SUB), :] = new + weight[g, pl.ds(at, SUB), :] * sums[g]

        each(level, body)

    def defect(level, ref, target):
        source, react, _, _, _, _, _ = levels_of[level]
        factor = 0.25**level

        def body(tile):
            at, here, sums = beside(ref, level, tile)
            mask = inside(tile, level) * factor
            for g in range(SUB >> level):
                diagonal = 6.0 * factor + react[g, pl.ds(at, SUB), :]
                value = source[g, pl.ds(at, SUB), :] - diagonal * here[g]
                target[g, pl.ds(at, SUB), :] = value + mask * sums[g]

        each(level, body)

    def coarsen(level, ref, target):
        reach = 1 << level
        odd = (lane & reach) != 0
        tiles = -(-(wide_z >> (level + 1)) // SUB)
        for tile in range(tiles):
            base = SUB + 2 * SUB * tile
            for g in range(SUB >> (level + 1)):
                value = None
                for part in range(2):
                    for phase in range(2):
                        piece = ref[2 * g + part, pl.ds(base + phase, SUB, stride=2), :]
                        value = piece if value is None else value + piece
                other = jnp.where(odd, pltpu.roll(value, reach, 1), pltpu.roll(value, LANES - reach, 1))
                target[g, SUB + tile * SUB : 2 * SUB + tile * SUB, :] = 0.125 * (value + other)

    def refine(level, lower, target):
        tiles = -(-(wide_z >> (level + 1)) // SUB)
        for tile in range(tiles):
            base = SUB + 2 * SUB * tile
            for g in range(SUB >> (level + 1)):
                value = lower[g, SUB + tile * SUB : 2 * SUB + tile * SUB, :]
                for part in range(2):
                    for phase in range(2):
                        where = (2 * g + part, pl.ds(base + phase, SUB, stride=2), whole)
                        target[where] = target[where] + value

    levels_of = [(src0, rea0) + tuple(levels[0][2:])] + [tuple(refs) for refs in levels[1:]]

    def vcycle(level):
        first, one, two, rest = levels_of[level][3:]
        prepare(level)
        if level == LEVELS - 1:
            now, later = first, one
            for _ in range(2 * SWEEPS - 1):
                sweep(level, now, later)
                now, later = later, (two if later is one else one)
            return now
        now, later = first, one
        for _ in range(SWEEPS - 1):
            sweep(level, now, later)
            now, later = later, (two if later is one else one)
        defect(level, now, rest)
        coarsen(level, rest, levels_of[level + 1][0])
        refine(level, vcycle(level + 1), now)
        for _ in range(SWEEPS):
            sweep(level, now, later)
            now, later = later, now
        return now

    for entry in z_faces[1]:
        await_recv(entry)
    for level in range(LEVELS):
        weigh(level)
        if level < LEVELS - 1:
            coarsen(level, levels_of[level][1], levels_of[level + 1][1])
    finish(gathering)

    total = counts[0] * counts[1] * counts[2]
    unknowns = inv_ref.shape[1]
    for number in range(total):
        i, rest = divmod(number, counts[1] * counts[2])
        j, k = divmod(rest, counts[2])
        rows[number : number + 1, :] = pall[i, j, k]
    column = iota((LANES, unknowns), 1)
    spread = one_hot(column - n_basis * quotient(column, n_basis) == iota((LANES, unknowns), 0))
    wide = dot(rows[...], spread)
    owner_low = iota((total, unknowns), 0) * n_basis
    owner_column = iota((total, unknowns), 1)
    owned = (owner_column >= owner_low) & (owner_column < owner_low + n_basis)
    vector = jnp.sum(jnp.where(owned, wide, 0.0), axis=0, keepdims=True)
    coefficients = jnp.sum(inverse[...] * vector, axis=1, keepdims=True)
    coarse = dot(basis_xy, coefficients * basis_z, ((0,), (0,)))
    out_ref[...] = coarse.reshape(size_x, size_y, size_z)

    for entry in z_faces[0]:
        await_recv(entry)
    solved = vcycle(0)
    for group in range(SUB):
        block = solved[group, SUB + MARGIN : SUB + MARGIN + size_z, :].T
        for part in range(1, groups - 1):
            x = SUB * part + group - MARGIN
            start_at = part * wide_y + MARGIN
            out_ref[x] = out_ref[x] + block[start_at : start_at + size_y, :]

    for field in range(2):
        for entry in x_faces[field] + y_faces[field] + tuple(corners[field]) + z_faces[field]:
            await_send(entry)


def shards(counts, residual, reaction, basis_x, basis_y, basis_z, coarse_inverse):
    size_x, size_y, size_z = residual.shape
    wide_x, wide_y, wide_z = size_x + 2 * MARGIN, size_y + 2 * MARGIN, size_z + 2 * MARGIN
    assert wide_x // SUB * wide_y == LANES and wide_x % SUB == 0
    total = counts[0] * counts[1] * counts[2]
    vmem = pl.BlockSpec(memory_space=pltpu.VMEM)
    placed = pl.BlockSpec(memory_space=pl.ANY)
    tall = wide_z + 2 * SUB
    scratch = [
        pltpu.VMEM((2, wide_x, wide_y, size_z), jnp.float32),
        pltpu.VMEM((SUB, tall, LANES), jnp.float32),
        pltpu.VMEM((SUB, tall, LANES), jnp.float32),
        pltpu.VMEM(coarse_inverse.shape, jnp.float32),
        pltpu.SemaphoreType.DMA((3,)),
    ]
    for level in range(LEVELS):
        rows = -(-(wide_z >> level) // SUB) * SUB + 2 * SUB
        shape = (SUB >> level, rows, LANES) if level else (1, SUB, LANES)
        scratch += [pltpu.VMEM(shape, jnp.float32)] * 2
        shape = (SUB >> level, rows, LANES)
        scratch += [pltpu.VMEM(shape, jnp.float32)] * 5
    scratch += [
        pltpu.VMEM((*counts, 1, LANES), jnp.float32),
        pltpu.VMEM((total, LANES), jnp.float32),
        pltpu.SemaphoreType.DMA((20,)),
        pltpu.SemaphoreType.DMA((20,)),
        pltpu.SemaphoreType.DMA((3 * max(counts),)),
        pltpu.SemaphoreType.DMA((3 * max(counts),)),
    ]
    return pl.pallas_call(
        functools.partial(kernel, counts),
        out_shape=jax.ShapeDtypeStruct(residual.shape, jnp.float32),
        in_specs=[placed, placed, vmem, vmem, vmem, placed],
        out_specs=vmem,
        scratch_shapes=scratch,
        compiler_params=pltpu.CompilerParams(collective_id=0, has_side_effects=True),
    )(residual, reaction, basis_x, basis_y, basis_z, coarse_inverse)


def solution(mesh):
    counts = tuple(mesh.shape[axis] for axis in AXES)
    placed = (
        P("gx", "gy", "gz"),
        P("gx", "gy", "gz"),
        P(None, "gx"),
        P(None, "gy"),
        P(None, "gz"),
        P(AXES, None),
    )
    return jax.shard_map(
        functools.partial(shards, counts), mesh=mesh, in_specs=placed,
        out_specs=P(*AXES), check_vma=False,
    )
```
